8 devices in a mesh: rep: 2 (over z, y), rows: 4 (over x, core).
Axes of the slice: x: 2, y: 2, z: 1, core: 2. Of those that a mesh axis runs over, the one named last changes fastest.
Arguments:
- adjacency: bfloat16 [16384, 16384], P('rows', 'rep')
- block_mask: int32 [4, 4], replicated
- features: bfloat16 [16384, 128], P('rows')
- w_one: bfloat16 [128, 256], replicated
- w_two: bfloat16 [256, 172], replicated
Outputs:
- output: float32 [16384, 172], P('rows')
All inputs are finite; a program needn't handle non-finite values.
Results may differ from the reference program's by a relative error of at most 0.001.
Values are sent between devices in bfloat16 or wider.
A program may use at most 1 GiB of HBM per device.

```python
import jax
import jax.numpy as jnp
from jax import lax

ROWS = 4
BLOCK = 4096
F0 = 128
F1 = 256
F2 = 172

NODES = ROWS * BLOCK


def draw_mask(key):
    key_w, key_r = jax.random.split(key)
    weight = jax.random.randint(key_w, (ROWS,), 1, 5, dtype=jnp.int32)
    pair_draws = jnp.triu(jax.random.randint(key_r, (ROWS, ROWS), 0, 10, dtype=jnp.int32), 1)
    pair_draws = pair_draws + pair_draws.T
    block_ids = jnp.arange(ROWS)
    diag_pair = block_ids[:, None] == block_ids[None, :]
    keep_pair = pair_draws < weight[:, None] + weight[None, :]
    return (keep_pair | diag_pair).astype(jnp.int32)


def hash_rows(row_x, row_y, node_x, node_y):
    hash_bits = row_x[:, None] * node_x[None, :] + (row_y[:, None] ^ node_y[None, :])
    hash_bits = hash_bits ^ (hash_bits >> 15)
    hash_bits = hash_bits * 73244475
    return hash_bits ^ (hash_bits >> 13)


def build_adjacency(key, block_mask):
    key_x, key_y = jax.random.split(key)
    node_x = jax.random.randint(key_x, (NODES,), 0, 2 ** 30, dtype=jnp.int32)
    node_y = jax.random.randint(key_y, (NODES,), 0, 2 ** 30, dtype=jnp.int32)
    col_ids = jnp.arange(NODES)

    def edge_rows(blk_idx):
        row_start = blk_idx * BLOCK
        row_ids = row_start + jnp.arange(BLOCK)
        hash_bits = hash_rows(lax.dynamic_slice_in_dim(node_x, row_start, BLOCK), lax.dynamic_slice_in_dim(node_y, row_start, BLOCK), node_x, node_y)
        col_keep = jnp.repeat(block_mask[blk_idx], BLOCK) == 1
        self_loop = row_ids[:, None] == col_ids[None, :]
        linked = ((hash_bits & 7) == 0) & col_keep[None, :] & jnp.logical_not(self_loop)
        return (linked | self_loop).astype(jnp.float32)

    degree = lax.map(lambda blk_idx: jnp.sum(edge_rows(blk_idx), axis=1), jnp.arange(ROWS)).reshape(NODES)
    inv_root = lax.rsqrt(degree)

    def scaled_rows(blk_idx):
        row_scale = lax.dynamic_slice_in_dim(inv_root, blk_idx * BLOCK, BLOCK)
        return (edge_rows(blk_idx) * row_scale[:, None] * inv_root[None, :]).astype(jnp.bfloat16)

    adjacency = lax.map(scaled_rows, jnp.arange(ROWS)).reshape(NODES, NODES)
    return adjacency, jnp.mean(degree)


def setup_inputs(seed: int = 0) -> dict:
    key_mask, key_adj, key_feat, key_one, key_two = jax.random.split(jax.random.key(seed), 5)
    block_mask = draw_mask(key_mask)
    adjacency, mean_degree = build_adjacency(key_adj, block_mask)
    features = jax.random.normal(key_feat, (NODES, F0), jnp.float32).astype(jnp.bfloat16)
    w_one = (jax.random.normal(key_one, (F0, F1), jnp.float32) * jnp.sqrt(mean_degree / F0)).astype(jnp.bfloat16)
    w_two = (jax.random.normal(key_two, (F1, F2), jnp.float32) * (F1 ** -0.5)).astype(jnp.bfloat16)
    return {'adjacency': adjacency, 'block_mask': block_mask, 'features': features, 'w_one': w_one, 'w_two': w_two}


def reference(adjacency, block_mask, features, w_one, w_two):
    adj_blocks = adjacency.reshape(ROWS, BLOCK, NODES)

    def aggregate(feat_table):
        feat_width = feat_table.shape[1]
        feat_blocks = feat_table.reshape(ROWS, BLOCK, feat_width)

        def one_block(block_pair):
            adj_rows, mask_row = block_pair
            masked = (feat_blocks * mask_row.astype(feat_table.dtype)[:, None, None]).reshape(NODES, feat_width)
            return jnp.dot(adj_rows, masked, preferred_element_type=jnp.float32)

        return lax.map(one_block, (adj_blocks, block_mask)).reshape(NODES, feat_width)

    y_one = aggregate(features).astype(jnp.bfloat16)
    z_one = jnp.maximum(jnp.dot(y_one, w_one, preferred_element_type=jnp.float32), 0.0).astype(jnp.bfloat16)
    y_two = aggregate(z_one).astype(jnp.bfloat16)
    return jnp.dot(y_two, w_two, preferred_element_type=jnp.float32)
```

```python
import jax
import jax.numpy as jnp
from jax import lax
from jax.experimental import pallas as pl
from jax.experimental.pallas import tpu as pltpu
from jax.sharding import PartitionSpec as P

MESH = pl.DeviceIdType.MESH
BLK = 4096
CH = 256
NCH = BLK // CH
HALF = NCH // 2
NBUF = 3
F0 = 128
F1 = 256
F32 = jnp.float32
BF16 = jnp.bfloat16


def loop(lo, hi, fn):
    def body(idx, carry):
        fn(idx)
        return carry
    lax.fori_loop(lo, hi, body, 0)


def kernel(mask_ref, w1_ref, a_ref, h_ref, y2_ref,
           abuf_r, abuf_c, hbuf, ht, w1t, pbuf_s, pbuf_r, mbuf_s, mbuf_r, own1, ybuf, ybuf_i, z, zt,
           dfb, tms, tmr, own2, tfb, y2s,
           ar_sem, ac_sem, h_sem, hx_s, hx_r, pf_s, pf_r, mf_s, mf_r, pb_s, pb_r, mb_s, mb_r, yb_s, yb_r,
           df_s, df_r, tm_s, tm_r, tf_s, tf_r, ob_s, ob_r, out_sem):
    rep = lax.axis_index('rep')
    row = lax.axis_index('rows')
    chip_x = row // 2
    core = row % 2
    diag = chip_x == rep
    other = 1 - core
    partner = (rep, (1 - chip_x) * 2 + core)
    mate = (rep, chip_x * 2 + other)
    yside = (1 - rep, row)
    blk_own = rep * 2 + core
    blk_other = rep * 2 + other

    def remote(src, dst, send, recv, dev):
        return pltpu.make_async_remote_copy(src_ref=src, dst_ref=dst, send_sem=send, recv_sem=recv, device_id=dev, device_id_type=MESH)

    def row_copy(m, slot):
        return pltpu.make_async_copy(a_ref.at[pl.ds(pl.multiple_of(m * CH, CH), CH), :], abuf_r.at[slot], ar_sem.at[slot])

    def col_copy(q, slot, k):
        return pltpu.make_async_copy(a_ref.at[:, pl.ds(pl.multiple_of(k * BLK + q * CH, CH), CH)], abuf_c.at[slot, k], ac_sem.at[slot, k])

    def h_send():
        return remote(h_ref, hbuf.at[core], hx_s, hx_r, mate)

    def pf(r):
        return remote(pbuf_s.at[r], pbuf_r.at[r], pf_s.at[r], pf_r.at[r], partner)

    def mf(m):
        return remote(mbuf_s.at[m], mbuf_r.at[m], mf_s.at[m], mf_r.at[m], mate)

    def pb(m, r):
        return remote(ybuf.at[core, m], ybuf.at[core, m], pb_s.at[r], pb_r.at[r], partner)

    def mb_out(m):
        return remote(ybuf.at[core, m], ybuf.at[core, m], mb_s.at[m], mb_r.at[m], mate)

    def mb_in(m):
        return remote(ybuf.at[other, m], ybuf.at[other, m], mb_s.at[m], mb_r.at[m], mate)

    def yb(m):
        return remote(ybuf.at[core, m], ybuf_i.at[m], yb_s.at[m], yb_r.at[m], yside)

    def df(m):
        return remote(dfb.at[m], dfb.at[m], df_s.at[m], df_r.at[m], yside)

    def tm(m):
        return remote(tms.at[m], tmr.at[m], tm_s.at[m], tm_r.at[m], mate)

    def tf(m):
        return remote(tfb.at[m], tfb.at[m], tf_s.at[m], tf_r.at[m], partner)

    def out_rows(m):
        return y2_ref.at[pl.ds(pl.multiple_of(m * CH, CH), CH), :]

    def ob(m):
        return remote(y2s.at[m], out_rows(m), ob_s.at[m], ob_r.at[m], yside)

    def out_copy(m):
        return pltpu.make_async_copy(y2s.at[m], out_rows(m), out_sem.at[m])

    def mask_of(dst_blk, src_blk):
        return mask_ref[dst_blk, src_blk].astype(F32)

    def hidden_rows(k, m):
        hid = jnp.maximum(jnp.dot(ybuf[k, m], w1_ref[...], preferred_element_type=F32), 0.0)
        z[pl.ds(pl.multiple_of(k * BLK + m * CH, CH), CH), :] = (hid * mask_of(row, rep * 2 + k)).astype(BF16)

    def barrier():
        sem = pltpu.get_barrier_semaphore()
        for dev in (partner, mate, yside):
            pl.semaphore_signal(sem, inc=1, device_id=dev, device_id_type=MESH)
        pl.semaphore_wait(sem, 3)

    h_own = pltpu.make_async_copy(h_ref, hbuf.at[core], h_sem)
    h_own.start()

    @pl.when(diag)
    def _():
        for t in range(NBUF):
            row_copy(t + HALF, t).start()

    @pl.when(jnp.logical_not(diag))
    def _():
        for t in range(NBUF):
            for k in range(2):
                col_copy(t, t, k).start()

    barrier()

    @pl.when(diag)
    def _():
        h_send().start()

        def chunk_at(t):
            first = (t + HALF) % NCH
            second = t - NCH
            return jnp.where(t < NCH, first, second // 2 + HALF * (second % 2))

        def next_load(t):
            nxt = t + NBUF

            @pl.when(nxt < 2 * NCH)
            def _():
                row_copy(chunk_at(nxt), nxt % NBUF).start()

        h_own.wait()
        hbuf[core] = (hbuf[core].astype(F32) * mask_of(row, blk_own)).astype(BF16)
        remote(h_ref, hbuf.at[other], hx_s, hx_r, mate).wait_recv()
        hbuf[other] = (hbuf[other].astype(F32) * mask_of(row, blk_other)).astype(BF16)

        def product1(t):
            slot = t % NBUF
            row_copy(0, slot).wait()
            return jnp.dot(abuf_r[slot], hbuf[...].reshape(2 * BLK, F0), preferred_element_type=F32)

        def send_half(t):
            pbuf_s[t] = product1(t)
            pf(t).start()
            next_load(t)
        loop(0, HALF, send_half)

        def keep_half(r):
            t = r + HALF
            part = product1(t)
            next_load(t)
            pf(r).wait_recv()
            ybuf[core, r] = (part + pbuf_r[r]).astype(BF16)
            pb(r, r).start()
            yb(r).start()
            mb_out(r).start()
            hidden_rows(core, r)
        loop(0, HALF, keep_half)

        def relay(r):
            m = r + HALF
            pb(m, r).wait_recv()
            yb(m).start()
            mb_out(m).start()
            hidden_rows(core, m)
            mb_in(r).wait_recv()
            hidden_rows(other, r)
        loop(0, HALF, relay)

        def rest(r):
            mb_in(r + HALF).wait_recv()
            hidden_rows(other, r + HALF)
        loop(0, HALF, rest)

        def layer2(s):
            t = s + NCH
            slot = t % NBUF
            m = chunk_at(t)
            row_copy(0, slot).wait()
            part = jnp.dot(abuf_r[slot], z[...], preferred_element_type=F32)
            next_load(t)
            half = s // 2

            def finish(got):
                y2s[m] = (part + got).astype(BF16)

            @pl.when(s % 2 == 0)
            def _():
                df(half).wait_recv()
                finish(dfb[half])

            @pl.when(s % 2 == 1)
            def _():
                tf(half).wait_recv()
                finish(tfb[half])
            ob(m).start()
            out_copy(m).start()
        loop(0, NCH, layer2)

        h_send().wait_send()

        def drain_half(r):
            pf(r).wait_send()
            pb(r, r).wait_send()
        loop(0, HALF, drain_half)

        def drain(m):
            yb(m).wait_send()
            mb_out(m).wait_send()
            ob(m).wait_send()
            out_copy(m).wait()
        loop(0, NCH, drain)

    @pl.when(jnp.logical_not(diag))
    def _():
        def next_cols(t):
            nxt = t + NBUF

            @pl.when(nxt < NCH + HALF)
            def _():
                q = jnp.where(nxt < NCH, nxt, nxt - HALF)
                for k in range(2):
                    col_copy(q, nxt % NBUF, k).start()

        def cols_wait(slot):
            for k in range(2):
                col_copy(0, slot, k).wait()

        w1t[...] = w1_ref[...].astype(F32).T.astype(BF16)
        h_own.wait()

        def turn(m):
            piece = hbuf[core, pl.ds(pl.multiple_of(m * CH, CH), CH), :]
            ht[:, pl.ds(pl.multiple_of(m * CH, CH), CH)] = piece.astype(F32).T.astype(BF16)
        loop(0, NCH, turn)

        mask_own = mask_of(blk_own, row)
        mask_other = mask_of(blk_other, row)

        def produce1(t):
            slot = t % NBUF
            cols_wait(slot)
            mbuf_s[t] = jnp.dot(ht[...], abuf_c[slot, other], preferred_element_type=F32) * mask_other
            mf(t).start()
            own1[t % 2] = jnp.dot(ht[...], abuf_c[slot, core], preferred_element_type=F32) * mask_own
            next_cols(t)

        def combine1(t):
            mf(t).wait_recv()
            return (own1[t % 2] + mbuf_r[t]).T

        def combine_send(t):
            pbuf_s[t] = combine1(t)
            pf(t).start()

        def combine_keep(r):
            m = r + HALF
            part = combine1(m)
            pf(r).wait_recv()
            ybuf[core, m] = (part + pbuf_r[r]).astype(BF16)
            pb(m, r).start()
            mb_out(m).start()
            hidden_rows(core, m)

        produce1(0)

        def send_half(t):
            produce1(t + 1)
            combine_send(t)
        loop(0, HALF, send_half)

        def keep_half(r):
            produce1(r + HALF + 1)
            combine_keep(r)
        loop(0, HALF - 1, keep_half)
        combine_keep(HALF - 1)

        for v in range(NBUF):
            row_copy(v, v).start()

        def hidden_turned(m):
            yb(m).wait_recv()
            hid = lax.dot_general(w1t[...], ybuf_i[m], (((1,), (1,)), ((), ())), preferred_element_type=F32)
            zt[:, pl.ds(pl.multiple_of(m * CH, CH), CH)] = jnp.maximum(hid, 0.0).astype(BF16)

        def relay(r):
            pb(r, r).wait_recv()
            mb_out(r).start()
            hidden_rows(core, r)
            mb_in(r + HALF).wait_recv()
            hidden_rows(other, r + HALF)
            hidden_turned(r)
        loop(0, HALF, relay)

        def rest(r):
            mb_in(r).wait_recv()
            hidden_rows(other, r)
            hidden_turned(r + HALF)
        loop(0, HALF, rest)

        def produce2(m):
            slot_r = m % NBUF
            row_copy(0, slot_r).wait()
            dfb[m] = jnp.dot(abuf_r[slot_r], z[...], preferred_element_type=F32)
            df(m).start()

            @pl.when(m + NBUF < HALF)
            def _():
                row_copy(m + NBUF, slot_r).start()
            t = m + NCH
            slot = t % NBUF
            cols_wait(slot)
            tms[m] = jnp.dot(zt[...], abuf_c[slot, other], preferred_element_type=F32) * mask_other
            tm(m).start()
            own2[m % 2] = jnp.dot(zt[...], abuf_c[slot, core], preferred_element_type=F32) * mask_own
            next_cols(t)

        def combine2(m):
            tm(m).wait_recv()
            tfb[m] = (own2[m % 2] + tmr[m]).T
            tf(m).start()

        produce2(0)

        def layer2(m):
            produce2(m + 1)
            combine2(m)
        loop(0, HALF - 1, layer2)
        combine2(HALF - 1)

        def receive(m):
            ob(m).wait_recv()
        loop(0, NCH, receive)

        def drain_half(r):
            pf(r).wait_send()
            pb(r + HALF, r).wait_send()
            df(r).wait_send()
            tm(r).wait_send()
            tf(r).wait_send()
        loop(0, HALF, drain_half)

        def drain(m):
            mf(m).wait_send()
            mb_out(m).wait_send()
        loop(0, NCH, drain)


def solution(mesh):
    def local_fn(adj_local, block_mask, feat_blk, w_one, w_two):
        dma = pltpu.SemaphoreType.DMA
        y_two = pl.pallas_call(
            kernel,
            out_shape=jax.ShapeDtypeStruct((BLK, F1), BF16),
            in_specs=[pl.BlockSpec(memory_space=pltpu.SMEM), pl.BlockSpec(memory_space=pltpu.VMEM), pl.BlockSpec(memory_space=pl.ANY), pl.BlockSpec(memory_space=pl.ANY)],
            out_specs=pl.BlockSpec(memory_space=pl.ANY),
            scratch_shapes=[
                pltpu.VMEM((NBUF, CH, 2 * BLK), BF16),
                pltpu.VMEM((NBUF, 2, BLK, CH), BF16),
                pltpu.VMEM((2, BLK, F0), BF16),
                pltpu.VMEM((F0, BLK), BF16),
                pltpu.VMEM((F1, F0), BF16),
                pltpu.VMEM((HALF, CH, F0), F32),
                pltpu.VMEM((HALF, CH, F0), F32),
                pltpu.VMEM((NCH, F0, CH), F32),
                pltpu.VMEM((NCH, F0, CH), F32),
                pltpu.VMEM((2, F0, CH), F32),
                pltpu.VMEM((2, NCH, CH, F0), BF16),
                pltpu.VMEM((NCH, CH, F0), BF16),
                pltpu.VMEM((2 * BLK, F1), BF16),
                pltpu.VMEM((F1, BLK), BF16),
                pltpu.VMEM((HALF, CH, F1), F32),
                pltpu.VMEM((HALF, F1, CH), F32),
                pltpu.VMEM((HALF, F1, CH), F32),
                pltpu.VMEM((2, F1, CH), F32),
                pltpu.VMEM((HALF, CH, F1), F32),
                pltpu.VMEM((NCH, CH, F1), BF16),
                dma((NBUF,)), dma((NBUF, 2)), dma, dma, dma,
                dma((HALF,)), dma((HALF,)), dma((NCH,)), dma((NCH,)), dma((HALF,)), dma((HALF,)),
                dma((NCH,)), dma((NCH,)), dma((NCH,)), dma((NCH,)),
                dma((HALF,)), dma((HALF,)), dma((HALF,)), dma((HALF,)), dma((HALF,)), dma((HALF,)),
                dma((NCH,)), dma((NCH,)), dma((NCH,)),
            ],
            compiler_params=pltpu.CompilerParams(collective_id=0, has_side_effects=True, vmem_limit_bytes=66 * 1000 * 1000),
        )(block_mask, w_one, adj_local, feat_blk)
        return jnp.dot(y_two, w_two, preferred_element_type=F32)

    return jax.shard_map(local_fn, mesh=mesh, in_specs=(P('rows', 'rep'), P(), P('rows', None), P(), P()), out_specs=P('rows', None), check_vma=False)
```

```python
import jax
import jax.numpy as jnp
from jax import lax
from jax.experimental import pallas as pl
from jax.experimental.pallas import tpu as pltpu
from jax.sharding import PartitionSpec as P

MESH = pl.DeviceIdType.MESH
BLK = 4096
CH = 256
NCH = BLK // CH
HALF = NCH // 2
NBUF = 3
PC = 128
NPC = CH // PC
F0 = 128
F1 = 256
F32 = jnp.float32
BF16 = jnp.bfloat16


def loop(lo, hi, fn):
    def body(idx, carry):
        fn(idx)
        return carry
    lax.fori_loop(lo, hi, body, 0)


def kernel(mask_ref, w1_ref, a_ref, h_ref, y2_ref,
           abuf_r, abuf_c, hbuf, ht, w1t, pbuf_s, pbuf_r, mbuf_s, mbuf_r, own1, ybuf, ybuf_i, z, zt,
           dfb, tms, tmr, acc2, tfb, y2s,
           ar_sem, ac_sem, h_sem, hx_s, hx_r, pf_s, pf_r, mf_s, mf_r, pb_s, pb_r, mb_s, mb_r, yb_s, yb_r,
           df_s, df_r, tm_s, tm_r, tf_s, tf_r, ob_s, ob_r, out_sem):
    rep = lax.axis_index('rep')
    row = lax.axis_index('rows')
    chip_x = row // 2
    core = row % 2
    diag = chip_x == rep
    other = 1 - core
    partner = (rep, (1 - chip_x) * 2 + core)
    mate = (rep, chip_x * 2 + other)
    yside = (1 - rep, row)
    blk_own = rep * 2 + core
    blk_other = rep * 2 + other

    def remote(src, dst, send, recv, dev):
        return pltpu.make_async_remote_copy(src_ref=src, dst_ref=dst, send_sem=send, recv_sem=recv, device_id=dev, device_id_type=MESH)

    def row_copy(m, slot):
        return pltpu.make_async_copy(a_ref.at[pl.ds(pl.multiple_of(m * CH, CH), CH), :], abuf_r.at[slot], ar_sem.at[slot])

    def col_copy(q, slot, k):
        return pltpu.make_async_copy(a_ref.at[:, pl.ds(pl.multiple_of(k * BLK + q * CH, CH), CH)], abuf_c.at[slot, k], ac_sem.at[slot, k])

    def h_send():
        return remote(h_ref, hbuf.at[core], hx_s, hx_r, mate)

    def pf(r):
        return remote(pbuf_s.at[r], pbuf_r.at[r], pf_s.at[r], pf_r.at[r], partner)

    def mf(m):
        return remote(mbuf_s.at[m], mbuf_r.at[m], mf_s.at[m], mf_r.at[m], mate)

    def pb(m, r):
        return remote(ybuf.at[core, m], ybuf.at[core, m], pb_s.at[r], pb_r.at[r], partner)

    def mb_out(m):
        return remote(ybuf.at[core, m], ybuf.at[core, m], mb_s.at[m], mb_r.at[m], mate)

    def mb_in(m):
        return remote(ybuf.at[other, m], ybuf.at[other, m], mb_s.at[m], mb_r.at[m], mate)

    def yb(m):
        return remote(ybuf.at[core, m], ybuf_i.at[m], yb_s.at[m], yb_r.at[m], yside)

    def df(m, p):
        part = dfb.at[m, pl.ds(p * PC, PC), :]
        return remote(part, part, df_s.at[m, p], df_r.at[m, p], yside)

    def tm(m):
        return remote(tms.at[m], tmr.at[m], tm_s.at[m], tm_r.at[m], mate)

    def tf(m, p):
        part = tfb.at[m, pl.ds(p * PC, PC), :]
        return remote(part, part, tf_s.at[m, p], tf_r.at[m, p], partner)

    def out_rows(m, p):
        return y2_ref.at[pl.ds(pl.multiple_of(m * CH + p * PC, PC), PC), :]

    def ob(m, p):
        return remote(y2s.at[m, pl.ds(p * PC, PC), :], out_rows(m, p), ob_s.at[m, p], ob_r.at[m, p], yside)

    def out_copy(m, p):
        return pltpu.make_async_copy(y2s.at[m, pl.ds(p * PC, PC), :], out_rows(m, p), out_sem.at[m, p])

    def mask_of(dst_blk, src_blk):
        return mask_ref[dst_blk, src_blk].astype(F32)

    def hidden_rows(k, m):
        hid = jnp.maximum(jnp.dot(ybuf[k, m], w1_ref[...], preferred_element_type=F32), 0.0)
        z[pl.ds(pl.multiple_of(k * BLK + m * CH, CH), CH), :] = (hid * mask_of(row, rep * 2 + k)).astype(BF16)

    def barrier():
        sem = pltpu.get_barrier_semaphore()
        for dev in (partner, mate, yside):
            pl.semaphore_signal(sem, inc=1, device_id=dev, device_id_type=MESH)
        pl.semaphore_wait(sem, 3)

    h_own = pltpu.make_async_copy(h_ref, hbuf.at[core], h_sem)
    h_own.start()

    def first_loads(lo, hi):
        @pl.when(diag)
        def _():
            for t in range(lo, hi):
                row_copy(t + HALF, t).start()

        @pl.when(jnp.logical_not(diag))
        def _():
            for t in range(lo, hi):
                for k in range(2):
                    col_copy(t, t, k).start()

    first_loads(0, 1)
    barrier()

    @pl.when(diag)
    def _():
        h_send().start()

        def chunk_at(t):
            first = (t + HALF) % NCH
            second = t - NCH
            return jnp.where(t < NCH, first, second // 2 + HALF * (second % 2))

        def next_load(t):
            nxt = t + NBUF

            @pl.when(nxt < 2 * NCH)
            def _():
                row_copy(chunk_at(nxt), nxt % NBUF).start()

        h_own.wait()
        first_loads(1, NBUF)

        def product1_of(slot, k, dst):
            cols = pl.ds(pl.multiple_of(k * BLK, BLK), BLK)
            return jnp.dot(abuf_r[slot, :, cols], hbuf[k], preferred_element_type=F32) * mask_of(dst, rep * 2 + k)

        def product1(t):
            slot = t % NBUF
            row_copy(0, slot).wait()
            return product1_of(slot, 0, row) + product1_of(slot, 1, row)

        row_copy(0, 0).wait()
        pbuf_s[0] = product1_of(0, core, row)
        remote(h_ref, hbuf.at[other], hx_s, hx_r, mate).wait_recv()
        pbuf_s[0] = pbuf_s[0] + product1_of(0, other, row)
        pf(0).start()
        next_load(0)

        def send_half(t):
            pbuf_s[t] = product1(t)
            pf(t).start()
            next_load(t)
        loop(1, HALF, send_half)

        def keep_half(r):
            t = r + HALF
            part = product1(t)
            next_load(t)
            pf(r).wait_recv()
            ybuf[core, r] = (part + pbuf_r[r]).astype(BF16)
            pb(r, r).start()
            yb(r).start()
            mb_out(r).start()
            hidden_rows(core, r)
        loop(0, HALF, keep_half)

        def relay(r):
            m = r + HALF
            pb(m, r).wait_recv()
            yb(m).start()
            mb_out(m).start()
            hidden_rows(core, m)
            mb_in(r).wait_recv()
            hidden_rows(other, r)
        loop(0, HALF, relay)

        def rest(r):
            mb_in(r + HALF).wait_recv()
            hidden_rows(other, r + HALF)
        loop(0, HALF, rest)

        def product2(s):
            t = s + NCH
            slot = t % NBUF
            row_copy(0, slot).wait()
            acc2[s % 2] = jnp.dot(abuf_r[slot], z[...], preferred_element_type=F32)
            next_load(t)

        def finish(s):
            m = chunk_at(s + NCH)
            half = s // 2
            for p in range(NPC):
                rows = pl.ds(p * PC, PC)

                @pl.when(s % 2 == 0)
                def _():
                    df(half, p).wait_recv()
                    y2s[m, rows, :] = (acc2[s % 2, rows, :] + dfb[half, rows, :]).astype(BF16)

                @pl.when(s % 2 == 1)
                def _():
                    tf(half, p).wait_recv()
                    y2s[m, rows, :] = (acc2[s % 2, rows, :] + tfb[half, rows, :]).astype(BF16)
                ob(m, p).start()
                out_copy(m, p).start()

        product2(0)

        def layer2(s):
            product2(s + 1)
            finish(s)
        loop(0, NCH - 1, layer2)
        finish(NCH - 1)

        h_send().wait_send()

        def drain_half(r):
            pf(r).wait_send()
            pb(r, r).wait_send()
        loop(0, HALF, drain_half)

        def drain(m):
            yb(m).wait_send()
            mb_out(m).wait_send()
            for p in range(NPC):
                ob(m, p).wait_send()
                out_copy(m, p).wait()
        loop(0, NCH, drain)

    @pl.when(jnp.logical_not(diag))
    def _():
        def next_cols(t):
            nxt = t + NBUF

            @pl.when(nxt < NCH + HALF)
            def _():
                q = jnp.where(nxt < NCH, nxt, nxt - HALF)
                for k in range(2):
                    col_copy(q, nxt % NBUF, k).start()

        def cols_wait(slot):
            for k in range(2):
                col_copy(0, slot, k).wait()

        h_own.wait()

        def turn(m):
            piece = hbuf[core, pl.ds(pl.multiple_of(m * CH, CH), CH), :]
            ht[:, pl.ds(pl.multiple_of(m * CH, CH), CH)] = piece.astype(F32).T.astype(BF16)
        loop(0, NCH, turn)

        mask_own = mask_of(blk_own, row)
        mask_other = mask_of(blk_other, row)

        def produce1_other(t):
            slot = t % NBUF
            cols_wait(slot)
            mbuf_s[t] = jnp.dot(ht[...], abuf_c[slot, other], preferred_element_type=F32) * mask_other
            mf(t).start()

        def produce1_own(t):
            own1[t % 2] = jnp.dot(ht[...], abuf_c[t % NBUF, core], preferred_element_type=F32) * mask_own
            next_cols(t)

        def combine1(t):
            mf(t).wait_recv()
            return (own1[t % 2] + mbuf_r[t]).T

        def combine_send(t):
            pbuf_s[t] = combine1(t)
            pf(t).start()

        def combine_keep(r):
            m = r + HALF
            part = combine1(m)
            pf(r).wait_recv()
            ybuf[core, m] = (part + pbuf_r[r]).astype(BF16)
            pb(m, r).start()
            mb_out(m).start()
            hidden_rows(core, m)

        produce1_other(0)
        first_loads(1, NBUF)
        produce1_own(0)

        def send_half(t):
            produce1_other(t + 1)
            combine_send(t)
            produce1_own(t + 1)
        loop(0, HALF, send_half)

        def keep_half(r):
            produce1_other(r + HALF + 1)
            combine_keep(r)
            produce1_own(r + HALF + 1)
        loop(0, HALF - 1, keep_half)
        combine_keep(HALF - 1)
        w1t[...] = w1_ref[...].astype(F32).T.astype(BF16)

        for v in range(NBUF):
            row_copy(v, v).start()

        def hidden_turned(m):
            yb(m).wait_recv()
            hid = lax.dot_general(w1t[...], ybuf_i[m], (((1,), (1,)), ((), ())), preferred_element_type=F32)
            zt[:, pl.ds(pl.multiple_of(m * CH, CH), CH)] = jnp.maximum(hid, 0.0).astype(BF16)

        def relay(r):
            pb(r, r).wait_recv()
            mb_out(r).start()
            hidden_rows(core, r)
            mb_in(r + HALF).wait_recv()
            hidden_rows(other, r + HALF)
            hidden_turned(r)
        loop(0, HALF, relay)

        def rest(r):
            mb_in(r).wait_recv()
            hidden_rows(other, r)
        loop(0, HALF, rest)

        def direct(m):
            slot = m % NBUF
            row_copy(0, slot).wait()
            dfb[m] = jnp.dot(abuf_r[slot], z[...], preferred_element_type=F32)
            for p in range(NPC):
                df(m, p).start()

            @pl.when(m + NBUF < HALF)
            def _():
                row_copy(m + NBUF, slot).start()

        def turned_other(m):
            slot = (m + NCH) % NBUF
            cols_wait(slot)
            tms[m] = jnp.dot(zt[...], abuf_c[slot, other], preferred_element_type=F32) * mask_other
            tm(m).start()

        def turned_own(m):
            t = m + NCH
            own = jnp.dot(zt[...], abuf_c[t % NBUF, core], preferred_element_type=F32) * mask_own
            next_cols(t)
            acc2[0] = own
            tm(m).wait_recv()
            tfb[m] = (acc2[0] + tmr[m]).T
            for p in range(NPC):
                tf(m, p).start()

        direct(0)
        loop(HALF, NCH, hidden_turned)
        turned_other(0)
        turned_own(0)

        def layer2(m):
            turned_other(m)
            direct(m)
            turned_own(m)
        loop(1, HALF, layer2)

        def receive(m):
            for p in range(NPC):
                ob(m, p).wait_recv()
        loop(0, NCH, receive)

        def drain_half(r):
            pf(r).wait_send()
            pb(r + HALF, r).wait_send()
            tm(r).wait_send()
            for p in range(NPC):
                df(r, p).wait_send()
                tf(r, p).wait_send()
        loop(0, HALF, drain_half)

        def drain(m):
            mf(m).wait_send()
            mb_out(m).wait_send()
        loop(0, NCH, drain)


def solution(mesh):
    def local_fn(adj_local, block_mask, feat_blk, w_one, w_two):
        dma = pltpu.SemaphoreType.DMA
        y_two = pl.pallas_call(
            kernel,
            out_shape=jax.ShapeDtypeStruct((BLK, F1), BF16),
            in_specs=[pl.BlockSpec(memory_space=pltpu.SMEM), pl.BlockSpec(memory_space=pltpu.VMEM), pl.BlockSpec(memory_space=pl.ANY), pl.BlockSpec(memory_space=pl.ANY)],
            out_specs=pl.BlockSpec(memory_space=pl.ANY),
            scratch_shapes=[
                pltpu.VMEM((NBUF, CH, 2 * BLK), BF16),
                pltpu.VMEM((NBUF, 2, BLK, CH), BF16),
                pltpu.VMEM((2, BLK, F0), BF16),
                pltpu.VMEM((F0, BLK), BF16),
                pltpu.VMEM((F1, F0), BF16),
                pltpu.VMEM((HALF, CH, F0), F32),
                pltpu.VMEM((HALF, CH, F0), F32),
                pltpu.VMEM((NCH, F0, CH), F32),
                pltpu.VMEM((NCH, F0, CH), F32),
                pltpu.VMEM((2, F0, CH), F32),
                pltpu.VMEM((2, NCH, CH, F0), BF16),
                pltpu.VMEM((NCH, CH, F0), BF16),
                pltpu.VMEM((2 * BLK, F1), BF16),
                pltpu.VMEM((F1, BLK), BF16),
                pltpu.VMEM((HALF, CH, F1), F32),
                pltpu.VMEM((HALF, F1, CH), F32),
                pltpu.VMEM((HALF, F1, CH), F32),
                pltpu.VMEM((2, F1, CH), F32),
                pltpu.VMEM((HALF, CH, F1), F32),
                pltpu.VMEM((NCH, CH, F1), BF16),
                dma((NBUF,)), dma((NBUF, 2)), dma, dma, dma,
                dma((HALF,)), dma((HALF,)), dma((NCH,)), dma((NCH,)), dma((HALF,)), dma((HALF,)),
                dma((NCH,)), dma((NCH,)), dma((NCH,)), dma((NCH,)),
                dma((HALF, NPC)), dma((HALF, NPC)), dma((HALF,)), dma((HALF,)), dma((HALF, NPC)), dma((HALF, NPC)),
                dma((NCH, NPC)), dma((NCH, NPC)), dma((NCH, NPC)),
            ],
            compiler_params=pltpu.CompilerParams(collective_id=0, has_side_effects=True, vmem_limit_bytes=66 * 1000 * 1000),
        )(block_mask, w_one, adj_local, feat_blk)
        return jnp.dot(y_two, w_two, preferred_element_type=F32)

    return jax.shard_map(local_fn, mesh=mesh, in_specs=(P('rows', 'rep'), P(), P('rows', None), P(), P()), out_specs=P('rows', None), check_vma=False)
```

```python
import jax
import jax.numpy as jnp
from jax import lax
from jax.experimental import pallas as pl
from jax.experimental.pallas import tpu as pltpu
from jax.sharding import PartitionSpec as P

MESH = pl.DeviceIdType.MESH
BLK = 4096
CH = 256
NCH = BLK // CH
HALF = NCH // 2
NBUF = 3
PC = 128
NPC = CH // PC
F0 = 128
F1 = 256
F32 = jnp.float32
BF16 = jnp.bfloat16


def loop(lo, hi, fn):
    def body(idx, carry):
        fn(idx)
        return carry
    lax.fori_loop(lo, hi, body, 0)


def kernel(mask_ref, w1_ref, a_ref, h_ref, y2_ref,
           abuf_r, abuf_c, hbuf, ht, w1t, pbuf_s, pbuf_r, mbuf_s, mbuf_r, own1, ybuf, ybuf_i, z, zt,
           dfb, tms, tmr, acc2, tfb,
           ar_sem, ac_sem, h_sem, hx_s, hx_r, pf_s, pf_r, mf_s, mf_r, pb_s, pb_r, mb_s, mb_r, yb_s, yb_r,
           df_s, df_r, tm_s, tm_r, tf_s, tf_r, ob_s, ob_r):
    rep = lax.axis_index('rep')
    row = lax.axis_index('rows')
    chip_x = row // 2
    core = row % 2
    diag = chip_x == rep
    other = 1 - core
    partner = (rep, (1 - chip_x) * 2 + core)
    mate = (rep, chip_x * 2 + other)
    yside = (1 - rep, row)
    blk_own = rep * 2 + core
    blk_other = rep * 2 + other

    def remote(src, dst, send, recv, dev):
        return pltpu.make_async_remote_copy(src_ref=src, dst_ref=dst, send_sem=send, recv_sem=recv, device_id=dev, device_id_type=MESH)

    def row_copy(m, slot):
        return pltpu.make_async_copy(a_ref.at[pl.ds(pl.multiple_of(m * CH, CH), CH), :], abuf_r.at[slot], ar_sem.at[slot])

    def col_copy(q, slot, k):
        return pltpu.make_async_copy(a_ref.at[:, pl.ds(pl.multiple_of(k * BLK + q * CH, CH), CH)], abuf_c.at[slot, k], ac_sem.at[slot, k])

    def h_send():
        return remote(hbuf.at[core], hbuf.at[core], hx_s, hx_r, mate)

    def pf(r):
        return remote(pbuf_s.at[r], pbuf_r.at[r], pf_s.at[r], pf_r.at[r], partner)

    def mf(m):
        return remote(mbuf_s.at[m], mbuf_r.at[m], mf_s.at[m], mf_r.at[m], mate)

    def pb(m, r):
        return remote(ybuf.at[core, m], ybuf.at[core, m], pb_s.at[r], pb_r.at[r], partner)

    def mb_out(m):
        return remote(ybuf.at[core, m], ybuf.at[core, m], mb_s.at[m], mb_r.at[m], mate)

    def mb_in(m):
        return remote(ybuf.at[other, m], ybuf.at[other, m], mb_s.at[m], mb_r.at[m], mate)

    def yb(m):
        return remote(ybuf.at[core, m], ybuf_i.at[m], yb_s.at[m], yb_r.at[m], yside)

    def df(m, p):
        part = dfb.at[m, pl.ds(p * PC, PC), :]
        return remote(part, part, df_s.at[m, p], df_r.at[m, p], yside)

    def tm(m):
        return remote(tms.at[m], tmr.at[m], tm_s.at[m], tm_r.at[m], mate)

    def tf(m, p):
        part = tfb.at[m, pl.ds(p * PC, PC), :]
        return remote(part, part, tf_s.at[m, p], tf_r.at[m, p], partner)

    def out_rows(m, p):
        return y2_ref.at[pl.ds(pl.multiple_of(m * CH + p * PC, PC), PC), :]

    def ob(m, p):
        return remote(out_rows(m, p), out_rows(m, p), ob_s.at[m, p], ob_r.at[m, p], yside)

    def mask_of(dst_blk, src_blk):
        return mask_ref[dst_blk, src_blk].astype(F32)

    def hidden_rows(k, m):
        hid = jnp.maximum(jnp.dot(ybuf[k, m], w1_ref[...], preferred_element_type=F32), 0.0)
        z[pl.ds(pl.multiple_of(k * BLK + m * CH, CH), CH), :] = (hid * mask_of(row, rep * 2 + k)).astype(BF16)

    barrier = pltpu.get_barrier_semaphore()
    for dev in (partner, mate, yside):
        pl.semaphore_signal(barrier, inc=1, device_id=dev, device_id_type=MESH)
    h_own = pltpu.make_async_copy(h_ref, hbuf.at[core], h_sem)
    h_own.start()

    def first_loads(lo, hi):
        @pl.when(diag)
        def _():
            for t in range(lo, hi):
                row_copy(t + HALF, t).start()

        @pl.when(jnp.logical_not(diag))
        def _():
            for t in range(lo, hi):
                for k in range(2):
                    col_copy(t, t, k).start()

    first_loads(0, 1)
    h_own.wait()
    first_loads(1, 2)

    @pl.when(jnp.logical_not(diag))
    def _():
        def turn(m):
            piece = hbuf[core, pl.ds(pl.multiple_of(m * CH, CH), CH), :]
            ht[:, pl.ds(pl.multiple_of(m * CH, CH), CH)] = piece.astype(F32).T.astype(BF16)
        loop(0, NCH, turn)

    pl.semaphore_wait(barrier, 3)

    @pl.when(diag)
    def _():
        h_send().start()

        def chunk_at(t):
            first = (t + HALF) % NCH
            second = t - NCH
            return jnp.where(t < NCH, first, second // 2 + HALF * (second % 2))

        def next_load(t):
            nxt = t + NBUF

            @pl.when(nxt < 2 * NCH)
            def _():
                row_copy(chunk_at(nxt), nxt % NBUF).start()

        def product1_of(slot, k, dst):
            cols = pl.ds(pl.multiple_of(k * BLK, BLK), BLK)
            return jnp.dot(abuf_r[slot, :, cols], hbuf[k], preferred_element_type=F32) * mask_of(dst, rep * 2 + k)

        def product1(t):
            slot = t % NBUF
            row_copy(0, slot).wait()
            return product1_of(slot, 0, row) + product1_of(slot, 1, row)

        row_copy(0, 0).wait()
        pbuf_s[0] = product1_of(0, core, row)
        first_loads(2, NBUF)
        remote(hbuf.at[other], hbuf.at[other], hx_s, hx_r, mate).wait_recv()
        pbuf_s[0] = pbuf_s[0] + product1_of(0, other, row)
        pf(0).start()
        next_load(0)

        def send_half(t):
            pbuf_s[t] = product1(t)
            pf(t).start()
            next_load(t)
        loop(1, HALF, send_half)

        def keep_half(r):
            t = r + HALF
            part = product1(t)
            next_load(t)
            pf(r).wait_recv()
            ybuf[core, r] = (part + pbuf_r[r]).astype(BF16)
            pb(r, r).start()
            yb(r).start()
            mb_out(r).start()
            hidden_rows(core, r)
        loop(0, HALF, keep_half)

        def relay(r):
            m = r + HALF
            pb(m, r).wait_recv()
            yb(m).start()
            mb_out(m).start()
            hidden_rows(core, m)
            mb_in(r).wait_recv()
            hidden_rows(other, r)
        loop(0, HALF, relay)

        def rest(r):
            mb_in(r + HALF).wait_recv()
            hidden_rows(other, r + HALF)
        loop(0, HALF, rest)

        def product2(s):
            t = s + NCH
            slot = t % NBUF
            row_copy(0, slot).wait()
            acc2[s % 2] = jnp.dot(abuf_r[slot], z[...], preferred_element_type=F32)
            next_load(t)

        def finish(s):
            m = chunk_at(s + NCH)
            half = s // 2
            for p in range(NPC):
                rows = pl.ds(p * PC, PC)
                dst = pl.ds(pl.multiple_of(m * CH + p * PC, PC), PC)

                @pl.when(s % 2 == 0)
                def _():
                    df(half, p).wait_recv()
                    y2_ref[dst, :] = (acc2[s % 2, rows, :] + dfb[half, rows, :]).astype(BF16)

                @pl.when(s % 2 == 1)
                def _():
                    tf(half, p).wait_recv()
                    y2_ref[dst, :] = (acc2[s % 2, rows, :] + tfb[half, rows, :]).astype(BF16)
                ob(m, p).start()

        product2(0)

        def layer2(s):
            product2(s + 1)
            finish(s)
        loop(0, NCH - 1, layer2)
        finish(NCH - 1)

        h_send().wait_send()

        def drain_half(r):
            pf(r).wait_send()
            pb(r, r).wait_send()
        loop(0, HALF, drain_half)

        def drain(m):
            yb(m).wait_send()
            mb_out(m).wait_send()
            for p in range(NPC):
                ob(m, p).wait_send()
        loop(0, NCH, drain)

    @pl.when(jnp.logical_not(diag))
    def _():
        def next_cols(t):
            nxt = t + NBUF

            @pl.when(nxt < NCH + HALF)
            def _():
                q = jnp.where(nxt < NCH, nxt, nxt - HALF)
                for k in range(2):
                    col_copy(q, nxt % NBUF, k).start()

        def cols_wait(slot):
            for k in range(2):
                col_copy(0, slot, k).wait()

        mask_own = mask_of(blk_own, row)
        mask_other = mask_of(blk_other, row)

        def produce1_other(t):
            slot = t % NBUF
            cols_wait(slot)
            mbuf_s[t] = jnp.dot(ht[...], abuf_c[slot, other], preferred_element_type=F32) * mask_other
            mf(t).start()

        def produce1_own(t):
            own1[t % 2] = jnp.dot(ht[...], abuf_c[t % NBUF, core], preferred_element_type=F32) * mask_own
            next_cols(t)

        def combine1(t):
            mf(t).wait_recv()
            return (own1[t % 2] + mbuf_r[t]).T

        def combine_send(t):
            pbuf_s[t] = combine1(t)
            pf(t).start()

        def combine_keep(r):
            m = r + HALF
            part = combine1(m)
            pf(r).wait_recv()
            ybuf[core, m] = (part + pbuf_r[r]).astype(BF16)
            pb(m, r).start()
            mb_out(m).start()
            hidden_rows(core, m)

        produce1_other(0)
        first_loads(2, NBUF)
        produce1_own(0)
        combine_send(0)
        produce1_other(1)
        produce1_own(1)

        def send_half(t):
            produce1_other(t + 1)
            combine_send(t)
            produce1_own(t + 1)
        loop(1, HALF, send_half)

        def keep_half(r):
            produce1_other(r + HALF + 1)
            combine_keep(r)
            produce1_own(r + HALF + 1)
        loop(0, HALF - 1, keep_half)
        combine_keep(HALF - 1)
        w1t[...] = w1_ref[...].astype(F32).T.astype(BF16)

        for v in range(NBUF):
            row_copy(v, v).start()

        def hidden_turned(m):
            yb(m).wait_recv()
            hid = lax.dot_general(w1t[...], ybuf_i[m], (((1,), (1,)), ((), ())), preferred_element_type=F32)
            zt[:, pl.ds(pl.multiple_of(m * CH, CH), CH)] = jnp.maximum(hid, 0.0).astype(BF16)

        def relay(r):
            pb(r, r).wait_recv()
            mb_out(r).start()
            hidden_rows(core, r)
            mb_in(r + HALF).wait_recv()
            hidden_rows(other, r + HALF)
            hidden_turned(r)
        loop(0, HALF, relay)

        def rest(r):
            mb_in(r).wait_recv()
            hidden_rows(other, r)
        loop(0, HALF, rest)

        def direct(m):
            slot = m % NBUF
            row_copy(0, slot).wait()
            dfb[m] = jnp.dot(abuf_r[slot], z[...], preferred_element_type=F32)
            for p in range(NPC):
                df(m, p).start()

            @pl.when(m + NBUF < HALF)
            def _():
                row_copy(m + NBUF, slot).start()

        def turned_other(m):
            slot = (m + NCH) % NBUF
            cols_wait(slot)
            tms[m] = jnp.dot(zt[...], abuf_c[slot, other], preferred_element_type=F32) * mask_other
            tm(m).start()

        def turned_own(m):
            t = m + NCH
            own = jnp.dot(zt[...], abuf_c[t % NBUF, core], preferred_element_type=F32) * mask_own
            next_cols(t)
            acc2[0] = own
            tm(m).wait_recv()
            tfb[m] = (acc2[0] + tmr[m]).T
            for p in range(NPC):
                tf(m, p).start()

        direct(0)
        loop(HALF, NCH, hidden_turned)
        turned_other(0)
        turned_own(0)

        def layer2(m):
            turned_other(m)
            direct(m)
            turned_own(m)
        loop(1, HALF, layer2)

        def receive(m):
            for p in range(NPC):
                ob(m, p).wait_recv()
        loop(0, NCH, receive)

        def drain_half(r):
            pf(r).wait_send()
            pb(r + HALF, r).wait_send()
            tm(r).wait_send()
            for p in range(NPC):
                df(r, p).wait_send()
                tf(r, p).wait_send()
        loop(0, HALF, drain_half)

        def drain(m):
            mf(m).wait_send()
            mb_out(m).wait_send()
        loop(0, NCH, drain)


def solution(mesh):
    def local_fn(adj_local, block_mask, feat_blk, w_one, w_two):
        dma = pltpu.SemaphoreType.DMA
        y_two = pl.pallas_call(
            kernel,
            out_shape=pltpu.VMEM((BLK, F1), BF16),
            in_specs=[pl.BlockSpec(memory_space=pltpu.SMEM), pl.BlockSpec(memory_space=pltpu.VMEM), pl.BlockSpec(memory_space=pl.ANY), pl.BlockSpec(memory_space=pl.ANY)],
            out_specs=pl.BlockSpec(memory_space=pltpu.VMEM),
            scratch_shapes=[
                pltpu.VMEM((NBUF, CH, 2 * BLK), BF16),
                pltpu.VMEM((NBUF, 2, BLK, CH), BF16),
                pltpu.VMEM((2, BLK, F0), BF16),
                pltpu.VMEM((F0, BLK), BF16),
                pltpu.VMEM((F1, F0), BF16),
                pltpu.VMEM((HALF, CH, F0), F32),
                pltpu.VMEM((HALF, CH, F0), F32),
                pltpu.VMEM((NCH, F0, CH), F32),
                pltpu.VMEM((NCH, F0, CH), F32),
                pltpu.VMEM((2, F0, CH), F32),
                pltpu.VMEM((2, NCH, CH, F0), BF16),
                pltpu.VMEM((NCH, CH, F0), BF16),
                pltpu.VMEM((2 * BLK, F1), BF16),
                pltpu.VMEM((F1, BLK), BF16),
                pltpu.VMEM((HALF, CH, F1), F32),
                pltpu.VMEM((HALF, F1, CH), F32),
                pltpu.VMEM((HALF, F1, CH), F32),
                pltpu.VMEM((2, F1, CH), F32),
                pltpu.VMEM((HALF, CH, F1), F32),
                dma((NBUF,)), dma((NBUF, 2)), dma, dma, dma,
                dma((HALF,)), dma((HALF,)), dma((NCH,)), dma((NCH,)), dma((HALF,)), dma((HALF,)),
                dma((NCH,)), dma((NCH,)), dma((NCH,)), dma((NCH,)),
                dma((HALF, NPC)), dma((HALF, NPC)), dma((HALF,)), dma((HALF,)), dma((HALF, NPC)), dma((HALF, NPC)),
                dma((NCH, NPC)), dma((NCH, NPC)),
            ],
            compiler_params=pltpu.CompilerParams(collective_id=0, has_side_effects=True, vmem_limit_bytes=56 * 2 ** 20),
        )(block_mask, w_one, adj_local, feat_blk)
        return jnp.dot(y_two, w_two, preferred_element_type=F32)

    return jax.shard_map(local_fn, mesh=mesh, in_specs=(P('rows', 'rep'), P(), P('rows', None), P(), P()), out_specs=P('rows', None), check_vma=False)
```

```python
import jax
import jax.numpy as jnp
from jax import lax
from jax.experimental import pallas as pl
from jax.experimental.pallas import tpu as pltpu
from jax.sharding import PartitionSpec as P

MESH = pl.DeviceIdType.MESH
BLK = 4096
CH = 256
NCH = BLK // CH
HALF = NCH // 2
NBUF = 3
PC = 128
NPC = CH // PC
F0 = 128
F1 = 256
F32 = jnp.float32
BF16 = jnp.bfloat16


def loop(lo, hi, fn):
    def body(idx, carry):
        fn(idx)
        return carry
    lax.fori_loop(lo, hi, body, 0)


def kernel(mask_ref, w1_ref, a_ref, h_ref, y2_ref,
           abuf_r, abuf_c, hbuf, ht, w1t, pbuf_s, pbuf_r, mbuf_s, mbuf_r, own1, ybuf, ybuf_i, z, zt,
           dfb, tms, tmr, acc2, tfb,
           ar_sem, ac_sem, h_sem, hx_s, hx_r, pf_s, pf_r, mf_s, mf_r, pb_s, pb_r, mb_s, mb_r, yb_s, yb_r,
           df_s, df_r, tm_s, tm_r, tf_s, tf_r, ob_s, ob_r):
    rep = lax.axis_index('rep')
    row = lax.axis_index('rows')
    chip_x = row // 2
    core = row % 2
    diag = chip_x == rep
    other = 1 - core
    partner = (rep, (1 - chip_x) * 2 + core)
    mate = (rep, chip_x * 2 + other)
    yside = (1 - rep, row)
    blk_own = rep * 2 + core
    blk_other = rep * 2 + other

    block = pl.when(row + rep < 64)

    def remote(src, dst, send, recv, dev):
        return pltpu.make_async_remote_copy(src_ref=src, dst_ref=dst, send_sem=send, recv_sem=recv, device_id=dev, device_id_type=MESH)

    def row_copy(m, slot):
        return pltpu.make_async_copy(a_ref.at[pl.ds(pl.multiple_of(m * CH, CH), CH), :], abuf_r.at[slot], ar_sem.at[slot])

    def col_copy(q, slot, k):
        return pltpu.make_async_copy(a_ref.at[:, pl.ds(pl.multiple_of(k * BLK + q * CH, CH), CH)], abuf_c.at[slot, k], ac_sem.at[slot, k])

    def h_send():
        return remote(hbuf.at[core], hbuf.at[core], hx_s, hx_r, mate)

    def pf(r):
        return remote(pbuf_s.at[r], pbuf_r.at[r], pf_s.at[r], pf_r.at[r], partner)

    def mf(m):
        return remote(mbuf_s.at[m], mbuf_r.at[m], mf_s.at[m], mf_r.at[m], mate)

    def pb(m, r):
        return remote(ybuf.at[core, m], ybuf.at[core, m], pb_s.at[r], pb_r.at[r], partner)

    def mb_out(m):
        return remote(ybuf.at[core, m], ybuf.at[core, m], mb_s.at[m], mb_r.at[m], mate)

    def mb_in(m):
        return remote(ybuf.at[other, m], ybuf.at[other, m], mb_s.at[m], mb_r.at[m], mate)

    def yb(m):
        return remote(ybuf.at[core, m], ybuf_i.at[m], yb_s.at[m], yb_r.at[m], yside)

    def df(m, p):
        part = dfb.at[m, pl.ds(p * PC, PC), :]
        return remote(part, part, df_s.at[m, p], df_r.at[m, p], yside)

    def tm(m):
        return remote(tms.at[m], tmr.at[m], tm_s.at[m], tm_r.at[m], mate)

    def tf(m, p):
        part = tfb.at[m, pl.ds(p * PC, PC), :]
        return remote(part, part, tf_s.at[m, p], tf_r.at[m, p], partner)

    def out_rows(m, p):
        return y2_ref.at[pl.ds(pl.multiple_of(m * CH + p * PC, PC), PC), :]

    def ob(m, p):
        return remote(out_rows(m, p), out_rows(m, p), ob_s.at[m, p], ob_r.at[m, p], yside)

    def mask_of(dst_blk, src_blk):
        return mask_ref[dst_blk, src_blk].astype(F32)

    def hidden_rows(k, m):
        hid = jnp.maximum(jnp.dot(ybuf[k, m], w1_ref[...], preferred_element_type=F32), 0.0)
        z[pl.ds(pl.multiple_of(k * BLK + m * CH, CH), CH), :] = (hid * mask_of(row, rep * 2 + k)).astype(BF16)

    barrier = pltpu.get_barrier_semaphore()
    for dev in (partner, mate, yside):
        pl.semaphore_signal(barrier, inc=1, device_id=dev, device_id_type=MESH)
    h_own = pltpu.make_async_copy(h_ref, hbuf.at[core], h_sem)
    h_own.start()

    def first_loads(lo, hi):
        @pl.when(diag)
        def _():
            for t in range(lo, hi):
                row_copy(t + HALF, t).start()

        @pl.when(jnp.logical_not(diag))
        def _():
            for t in range(lo, hi):
                for k in range(2):
                    col_copy(t, t, k).start()

    first_loads(0, 1)
    h_own.wait()
    first_loads(1, 2)

    @pl.when(jnp.logical_not(diag))
    def _():
        def turn(m):
            piece = hbuf[core, pl.ds(pl.multiple_of(m * CH, CH), CH), :]
            ht[:, pl.ds(pl.multiple_of(m * CH, CH), CH)] = piece.astype(F32).T.astype(BF16)
        loop(0, NCH, turn)

    pl.semaphore_wait(barrier, 3)

    @pl.when(diag)
    def _():
        h_send().start()

        def chunk_at(t):
            first = (t + HALF) % NCH
            second = t - NCH
            return jnp.where(t < NCH, first, second // 2 + HALF * (second % 2))

        def next_load(t):
            nxt = t + NBUF

            @pl.when(nxt < 2 * NCH)
            def _():
                row_copy(chunk_at(nxt), nxt % NBUF).start()

        def product1_of(slot, k, dst):
            cols = pl.ds(pl.multiple_of(k * BLK, BLK), BLK)
            return jnp.dot(abuf_r[slot, :, cols], hbuf[k], preferred_element_type=F32) * mask_of(dst, rep * 2 + k)

        def product1(t):
            slot = t % NBUF
            row_copy(0, slot).wait()
            return product1_of(slot, 0, row) + product1_of(slot, 1, row)

        row_copy(0, 0).wait()
        pbuf_s[0] = product1_of(0, core, row)
        first_loads(2, NBUF)
        remote(hbuf.at[other], hbuf.at[other], hx_s, hx_r, mate).wait_recv()
        pbuf_s[0] = pbuf_s[0] + product1_of(0, other, row)
        pf(0).start()
        next_load(0)

        def send_half(t):
            @block
            def _():
                pbuf_s[t] = product1(t)
                pf(t).start()
            next_load(t)
        loop(1, HALF, send_half)

        def keep_half(r):
            t = r + HALF
            @block
            def _():
                part = product1(t)
                pf(r).wait_recv()
                ybuf[core, r] = (part + pbuf_r[r]).astype(BF16)
                pb(r, r).start()
                yb(r).start()
                mb_out(r).start()
            next_load(t)
            hidden_rows(core, r)
        loop(0, HALF, keep_half)

        def relay(r):
            m = r + HALF
            @block
            def _():
                pb(m, r).wait_recv()
                yb(m).start()
                mb_out(m).start()

            @block
            def _():
                hidden_rows(core, m)
                mb_in(r).wait_recv()
                hidden_rows(other, r)
        loop(0, HALF, relay)

        def rest(r):
            mb_in(r + HALF).wait_recv()
            hidden_rows(other, r + HALF)
        loop(0, HALF, rest)

        def product2(s):
            t = s + NCH
            slot = t % NBUF
            row_copy(0, slot).wait()
            acc2[s % 2] = jnp.dot(abuf_r[slot], z[...], preferred_element_type=F32)
            next_load(t)

        def finish(s):
            m = chunk_at(s + NCH)
            half = s // 2
            for p in range(NPC):
                rows = pl.ds(p * PC, PC)
                dst = pl.ds(pl.multiple_of(m * CH + p * PC, PC), PC)

                @pl.when(s % 2 == 0)
                def _():
                    df(half, p).wait_recv()
                    y2_ref[dst, :] = (acc2[s % 2, rows, :] + dfb[half, rows, :]).astype(BF16)

                @pl.when(s % 2 == 1)
                def _():
                    tf(half, p).wait_recv()
                    y2_ref[dst, :] = (acc2[s % 2, rows, :] + tfb[half, rows, :]).astype(BF16)
                ob(m, p).start()

        product2(0)

        def layer2(s):
            product2(s + 1)
            finish(s)
        loop(0, NCH - 1, layer2)
        finish(NCH - 1)

        h_send().wait_send()

        def drain_half(r):
            pf(r).wait_send()
            pb(r, r).wait_send()
        loop(0, HALF, drain_half)

        def drain(m):
            yb(m).wait_send()
            mb_out(m).wait_send()
            for p in range(NPC):
                ob(m, p).wait_send()
        loop(0, NCH, drain)

    @pl.when(jnp.logical_not(diag))
    def _():
        def next_cols(t):
            nxt = t + NBUF

            @pl.when(nxt < NCH + HALF)
            def _():
                q = jnp.where(nxt < NCH, nxt, nxt - HALF)
                for k in range(2):
                    col_copy(q, nxt % NBUF, k).start()

        def cols_wait(slot):
            for k in range(2):
                col_copy(0, slot, k).wait()

        mask_own = mask_of(blk_own, row)
        mask_other = mask_of(blk_other, row)

        def produce1_other(t):
            slot = t % NBUF
            cols_wait(slot)

            @block
            def _():
                mbuf_s[t] = jnp.dot(ht[...], abuf_c[slot, other], preferred_element_type=F32) * mask_other
                mf(t).start()

        def produce1_own(t):
            @block
            def _():
                own1[t % 2] = jnp.dot(ht[...], abuf_c[t % NBUF, core], preferred_element_type=F32) * mask_own
            next_cols(t)

        def combine1(t):
            mf(t).wait_recv()
            return (own1[t % 2] + mbuf_r[t]).T

        def combine_send(t):
            @block
            def _():
                pbuf_s[t] = combine1(t)
                pf(t).start()

        def combine_keep(r):
            m = r + HALF

            @block
            def _():
                part = combine1(m)
                pf(r).wait_recv()
                ybuf[core, m] = (part + pbuf_r[r]).astype(BF16)
                pb(m, r).start()
                mb_out(m).start()

            @block
            def _():
                hidden_rows(core, m)

        produce1_other(0)
        first_loads(2, NBUF)
        produce1_own(0)
        combine_send(0)
        produce1_other(1)
        produce1_own(1)

        def send_half(t):
            produce1_other(t + 1)
            combine_send(t)
            produce1_own(t + 1)
        loop(1, HALF, send_half)

        def keep_half(r):
            produce1_other(r + HALF + 1)
            combine_keep(r)
            produce1_own(r + HALF + 1)
        loop(0, HALF - 1, keep_half)
        combine_keep(HALF - 1)
        w1t[...] = w1_ref[...].astype(F32).T.astype(BF16)

        for v in range(NBUF):
            row_copy(v, v).start()

        def hidden_turned(m):
            yb(m).wait_recv()
            hid = lax.dot_general(w1t[...], ybuf_i[m], (((1,), (1,)), ((), ())), preferred_element_type=F32)
            zt[:, pl.ds(pl.multiple_of(m * CH, CH), CH)] = jnp.maximum(hid, 0.0).astype(BF16)

        def relay(r):
            @block
            def _():
                pb(r, r).wait_recv()
                mb_out(r).start()
            hidden_rows(core, r)
            mb_in(r + HALF).wait_recv()
            hidden_rows(other, r + HALF)
            hidden_turned(r)
        loop(0, HALF, relay)

        def rest(r):
            mb_in(r).wait_recv()
            hidden_rows(other, r)
        loop(0, HALF, rest)

        def direct(m):
            slot = m % NBUF
            row_copy(0, slot).wait()

            @block
            def _():
                dfb[m] = jnp.dot(abuf_r[slot], z[...], preferred_element_type=F32)
                for p in range(NPC):
                    df(m, p).start()

            @pl.when(m + NBUF < HALF)
            def _():
                row_copy(m + NBUF, slot).start()

        def turned_other(m):
            slot = (m + NCH) % NBUF
            cols_wait(slot)

            @block
            def _():
                tms[m] = jnp.dot(zt[...], abuf_c[slot, other], preferred_element_type=F32) * mask_other
                tm(m).start()

        def turned_own(m):
            t = m + NCH

            @block
            def _():
                acc2[0] = jnp.dot(zt[...], abuf_c[t % NBUF, core], preferred_element_type=F32) * mask_own
            next_cols(t)

            @block
            def _():
                tm(m).wait_recv()
                tfb[m] = (acc2[0] + tmr[m]).T
                for p in range(NPC):
                    tf(m, p).start()

        direct(0)
        loop(HALF, NCH, hidden_turned)
        turned_other(0)
        turned_own(0)

        def layer2(m):
            turned_other(m)
            direct(m)
            turned_own(m)
        loop(1, HALF, layer2)

        def receive(m):
            for p in range(NPC):
                ob(m, p).wait_recv()
        loop(0, NCH, receive)

        def drain_half(r):
            pf(r).wait_send()
            pb(r + HALF, r).wait_send()
            tm(r).wait_send()
            for p in range(NPC):
                df(r, p).wait_send()
                tf(r, p).wait_send()
        loop(0, HALF, drain_half)

        def drain(m):
            mf(m).wait_send()
            mb_out(m).wait_send()
        loop(0, NCH, drain)


def solution(mesh):
    def local_fn(adj_local, block_mask, feat_blk, w_one, w_two):
        dma = pltpu.SemaphoreType.DMA
        y_two = pl.pallas_call(
            kernel,
            out_shape=pltpu.VMEM((BLK, F1), BF16),
            in_specs=[pl.BlockSpec(memory_space=pltpu.SMEM), pl.BlockSpec(memory_space=pltpu.VMEM), pl.BlockSpec(memory_space=pl.ANY), pl.BlockSpec(memory_space=pl.ANY)],
            out_specs=pl.BlockSpec(memory_space=pltpu.VMEM),
            scratch_shapes=[
                pltpu.VMEM((NBUF, CH, 2 * BLK), BF16),
                pltpu.VMEM((NBUF, 2, BLK, CH), BF16),
                pltpu.VMEM((2, BLK, F0), BF16),
                pltpu.VMEM((F0, BLK), BF16),
                pltpu.VMEM((F1, F0), BF16),
                pltpu.VMEM((HALF, CH, F0), F32),
                pltpu.VMEM((HALF, CH, F0), F32),
                pltpu.VMEM((NCH, F0, CH), F32),
                pltpu.VMEM((NCH, F0, CH), F32),
                pltpu.VMEM((2, F0, CH), F32),
                pltpu.VMEM((2, NCH, CH, F0), BF16),
                pltpu.VMEM((NCH, CH, F0), BF16),
                pltpu.VMEM((2 * BLK, F1), BF16),
                pltpu.VMEM((F1, BLK), BF16),
                pltpu.VMEM((HALF, CH, F1), F32),
                pltpu.VMEM((HALF, F1, CH), F32),
                pltpu.VMEM((HALF, F1, CH), F32),
                pltpu.VMEM((2, F1, CH), F32),
                pltpu.VMEM((HALF, CH, F1), F32),
                dma((NBUF,)), dma((NBUF, 2)), dma, dma, dma,
                dma((HALF,)), dma((HALF,)), dma((NCH,)), dma((NCH,)), dma((HALF,)), dma((HALF,)),
                dma((NCH,)), dma((NCH,)), dma((NCH,)), dma((NCH,)),
                dma((HALF, NPC)), dma((HALF, NPC)), dma((HALF,)), dma((HALF,)), dma((HALF, NPC)), dma((HALF, NPC)),
                dma((NCH, NPC)), dma((NCH, NPC)),
            ],
            compiler_params=pltpu.CompilerParams(collective_id=0, has_side_effects=True, vmem_limit_bytes=56 * 2 ** 20),
        )(block_mask, w_one, adj_local, feat_blk)
        return jnp.dot(y_two, w_two, preferred_element_type=F32)

    return jax.shard_map(local_fn, mesh=mesh, in_specs=(P('rows', 'rep'), P(), P('rows', None), P(), P()), out_specs=P('rows', None), check_vma=False)
```
